32 devices in a mesh: dp: 4 (over y, core), expert: 2 (over x), group: 4 (over z).
Axes of the slice: x: 2, y: 2, z: 4, core: 2. Of those that a mesh axis runs over, the one named last changes fastest.
Arguments:
- tokens: bfloat16 [256, 7168], P(('dp', 'group')), may hold values from -6 to 6
- expert_ids: int32 [256, 8], P(('dp', 'group')), may hold values from 0 to 255, all different within a row; in each aligned block of 16 rows (0 to 15, 16 to 31, ...) at most 2 rows name the same one
- gate_values: bfloat16 [256, 8], P(('dp', 'group')), may hold values from 0.099609375 to 1
- gate_up: bfloat16 [2, 7168, 2, 2048], P('expert', None, None, 'group'), may hold values from -0.0625 to 0.0625
- down_weight: bfloat16 [2, 2048, 7168], P('expert', 'group'), may hold values from -0.125 to 0.125
- shared_gate_up: bfloat16 [7168, 2, 2048], P('expert', None, 'group'), may hold values from -0.0625 to 0.0625
- shared_down: bfloat16 [2048, 7168], P('group', 'expert'), may hold values from -0.125 to 0.125
Outputs:
- mixed: bfloat16 [256, 7168], P(('dp', 'group'), 'expert')
The draws below stay inside these ranges and needn't reach their ends.
Inputs may be any that keep to these rules, and one draw needn't show every extreme that they name: `expert_ids`: each row names 8 different routed experts. In each aligned block of 16 rows (the rows of one device) no expert is named by more than 2 rows, and in some blocks one is named by exactly 2 rows.
All inputs are finite; a program needn't handle non-finite values.
Results may differ from the reference program's by a relative error of at most 0.028.
Values may be sent and summed in bfloat16 or wider, within the bound.
A program may use at most 128 MiB of HBM per device.

```python
import math
import jax
import jax.numpy as jnp
import numpy as np

D = 7168
FF = 2048
ROUTED = 256
TOPK = 8
TOK_DEV = 16
CAP = 2
SLOTS = 2
FF_DEV = 512
TOKENS = 256
N_GROUP = 4


def block_levels(rng, dims, pieces, smallest, top_value):
    gain, own = 1.0, jax.random.fold_in(rng, 6)
    for position, parts in pieces:
        heights = jnp.exp(jax.random.uniform(jax.random.fold_in(own, position), (parts,), jnp.float32, smallest / len(pieces), top_value / len(pieces)))
        gain = gain * jnp.repeat(heights, dims[position] // parts).reshape([-1 if axis == position else 1 for axis in range(len(dims))])
    return gain


def routed_block(stream_key, own, number, rows, number_of, top, limit, skew):
    ranking = jax.random.permutation(stream_key, number_of)
    crowded, common = portions_of(number_of, rows * top, limit, skew, True), portions_of(number_of, rows * top, limit, skew, False)
    places = jnp.arange(number_of)

    def named(tallies, rotation):
        used = int((tallies > 0).sum())
        fixed = max(1, used // 4)
        moved = fixed + (places - fixed + rotation * (used - fixed)) % max(1, number_of - fixed)
        return jnp.zeros((number_of,), jnp.int32).at[ranking[jnp.where(places < fixed, places, moved)]].set(jnp.asarray(tallies, jnp.int32))

    tallies = jnp.where(number % 4 == 0, named(crowded, number // 4), named(common, number - number // 4 - 1))
    mixed = jax.random.permutation(jax.random.fold_in(own, 3), number_of)
    source_of, sink = mixed[0:number_of // 2 * 2:2], mixed[1:number_of // 2 * 2:2]
    room = jnp.minimum(tallies[source_of] - 1, limit - tallies[sink]) // 2
    room = jnp.where((source_of == ranking[0]) | (sink == ranking[0]) | (tallies[sink] == 0), 0, jnp.maximum(room, 0))
    moved = jax.random.randint(jax.random.fold_in(own, 4), (number_of // 2,), 0, 1 << 20) % (room + 1)
    tallies = tallies.at[source_of].add(-moved).at[sink].add(moved)
    members = jnp.searchsorted(jnp.cumsum(tallies), jnp.arange(rows * top), side="right").astype(jnp.int32)
    table = members.reshape(top, rows).T
    table = table[jax.random.permutation(jax.random.fold_in(own, 1), rows)]
    rotation = jax.random.randint(jax.random.fold_in(own, 2), (rows, 1), 0, top)
    return jnp.take_along_axis(table, (jnp.arange(top)[None, :] + rotation) % top, axis=1)


def portions_of(amount, total, reach, lean, full):
    weights = [(1 << 20) // math.isqrt(rank ** lean) + 1 for rank in range(1, amount + 1)]
    largest = reach if full else min(reach, max(-(-total // amount), total * weights[0] // sum(weights)))
    least = 1 if total - largest >= amount - 1 else 0
    counts, rest = [largest] + [least] * (amount - 1), total - largest - least * (amount - 1)
    while rest > 0:
        movable = [i for i in range(1, amount) if counts[i] < largest] or [i for i in range(1, amount) if counts[i] < reach]
        pool, left = sum([weights[i] for i in movable]), rest
        for i in movable:
            more = min(reach - counts[i], max(1, left * weights[i] // pool), rest)
            counts[i] = counts[i] + more
            rest = rest - more
    return np.array(counts)


def centred(key, extent, width, bound, pieces=(), dtype=jnp.bfloat16):
    result = jax.random.normal(key, extent, jnp.float32) * width
    if len(pieces) > 0:
        result = block_levels(key, extent, pieces, -0.22, 0.18) * result
    return jnp.clip(result, min=-bound, max=bound).astype(dtype)


def setup_inputs(seed: int = 0) -> dict:
    streams_of = jax.random.split(jax.random.key(seed), 8)
    tokens = centred(streams_of[0], (TOKENS, D), 1.0, 6.0, ((0, 16),))
    expert_ids_keys = jax.random.split(jax.random.fold_in(streams_of[1], 1), TOKENS // TOK_DEV)
    expert_ids_turns = jax.random.permutation(jax.random.fold_in(streams_of[1], 3), TOKENS // TOK_DEV)
    expert_ids = jax.vmap(lambda own, number: routed_block(jax.random.fold_in(streams_of[1], 2), own, number, TOK_DEV, ROUTED, TOPK, CAP, 2))(expert_ids_keys, expert_ids_turns).reshape((TOKENS, TOPK))
    gate_values = jnp.clip(jnp.exp(math.log(1.0) - 2.306499 * jax.random.uniform(streams_of[2], (TOKENS, TOPK), jnp.float32) ** block_levels(streams_of[2], (TOKENS, TOPK), ((0, 16),), -0.2, 0.2)), 0.099609375, 1.0).astype(jnp.bfloat16)
    gate_up = centred(streams_of[3], (SLOTS, D, 2, FF), D ** -0.5, 0.0625, ((0, 2), (3, 4)))
    down_weight = centred(streams_of[4], (SLOTS, FF, D), FF ** -0.5, 0.125, ((0, 2), (1, 4)))
    shared_gate_up = centred(streams_of[5], (D, 2, FF), D ** -0.5, 0.0625, ((0, 2), (2, 4)))
    shared_down = centred(streams_of[6], (FF, D), FF ** -0.5, 0.125, ((0, 4), (1, 2)))
    return {"tokens": tokens, "expert_ids": expert_ids, "gate_values": gate_values, "gate_up": gate_up, "down_weight": down_weight, "shared_gate_up": shared_gate_up, "shared_down": shared_down}


def reference(tokens, expert_ids, gate_values, gate_up, down_weight, shared_gate_up, shared_down):
    accumulated = jnp.zeros((TOKENS, D), jnp.float32)
    for slot_index in range(SLOTS):
        chosen = expert_ids == slot_index
        slot_weight = jnp.sum(jnp.where(chosen, gate_values.astype(jnp.float32), jnp.float32(0.0)), axis=1)
        gate_part = jnp.dot(tokens, gate_up[slot_index, :, 0, :], preferred_element_type=jnp.float32)
        up_part = jnp.dot(tokens, gate_up[slot_index, :, 1, :], preferred_element_type=jnp.float32)
        hidden = (jax.nn.silu(gate_part) * up_part).astype(jnp.bfloat16)
        for block_index in range(N_GROUP):
            first_unit = block_index * FF_DEV
            product = jnp.dot(hidden[:, first_unit:first_unit + FF_DEV],
                              down_weight[slot_index, first_unit:first_unit + FF_DEV, :],
                              preferred_element_type=jnp.float32)
            slot_term = (product * slot_weight[:, None]).astype(jnp.bfloat16)
            accumulated = accumulated + slot_term.astype(jnp.float32)
    shared_gate = jnp.dot(tokens, shared_gate_up[:, 0, :], preferred_element_type=jnp.float32)
    shared_up = jnp.dot(tokens, shared_gate_up[:, 1, :], preferred_element_type=jnp.float32)
    shared_hidden = (jax.nn.silu(shared_gate) * shared_up).astype(jnp.bfloat16)
    for block_index in range(N_GROUP):
        first_unit = block_index * FF_DEV
        shared_term = jnp.dot(shared_hidden[:, first_unit:first_unit + FF_DEV],
                              shared_down[first_unit:first_unit + FF_DEV, :],
                              preferred_element_type=jnp.float32).astype(jnp.bfloat16)
        accumulated = accumulated + shared_term.astype(jnp.float32)
    return accumulated.astype(jnp.bfloat16)
```

```python
import functools

import jax
import jax.numpy as jnp
from jax import lax
from jax.experimental import pallas as pl
from jax.experimental.pallas import tpu as pltpu
from jax.sharding import PartitionSpec as P

MESH = pl.DeviceIdType.MESH
BF16, F32 = jnp.bfloat16, jnp.float32
CAP = 2
LANES = 128
DEPTH = 1792
scope = jax.named_scope


def line_order(count):
    orders = []
    for me in range(count):
        others = [j for j in range(count) if j != me]
        others.sort(key=lambda j: (abs(j - me), abs(2 * j - (count - 1))))
        orders.append([me] + others)
    return [[orders[me][k] for me in range(count)] for k in range(count)]


def choose(table, me):
    value = jnp.int32(0)
    for j, entry in enumerate(table):
        value = value + jnp.where(me == j, entry, 0)
    return value


def silu(value):
    return value / (1.0 + jnp.exp(-value))


def kernel(
    n_expert, n_group,
    tokens, ids_hbm, gates_hbm, gate_up, down, shared_gate_up, shared_down,
    out,
    w_routed, w_down, w_shared, w_shared_down,
    ids_all, gates,
    x_all, x_shared, rows_out, rows_all, x_routed,
    pre_own, pre_out, pre_in, term_out, term_in, routed_out, routed_in,
    routed_w_sem, down_w_sem, shared_w_sem, shared_down_w_sem, own_sem, ids_sem, gates_sem,
    x_send, x_recv, relay_send, ids_send, ids_recv, rows_send, rows_recv, pre_send, pre_recv,
    term_send, term_recv, routed_send, routed_recv,
):
    me_e, me_g = lax.axis_index("expert"), lax.axis_index("group")
    n_tokens, width = tokens.shape
    columns = x_all.shape[2]
    units = w_shared_down.shape[0]
    tiles = units // LANES
    pair = 2 if tiles % 2 == 0 else 1
    parts = 2 if columns % (2 * LANES) == 0 else 1
    part = columns // parts
    chunks = [pl.ds(c * part, part) for c in range(parts)]
    sources = [choose(table, me_g) for table in line_order(n_group)]

    def expert_at(distance):
        return lax.rem(me_e + n_expert + distance, n_expert)

    def group_at(distance):
        return lax.rem(me_g + n_group + distance, n_group)

    barrier = pltpu.get_barrier_semaphore()
    for d in range(n_expert):
        for s in range(n_group):
            if d or s:
                pl.semaphore_signal(
                    barrier, inc=1,
                    device_id={"expert": expert_at(d), "group": group_at(s)},
                    device_id_type=MESH,
                )

    own_columns = pl.ds(pl.multiple_of(me_e * columns, LANES), columns)
    own_copy = pltpu.make_async_copy(tokens.at[:, own_columns], x_all.at[me_g], own_sem)
    ids_copy = pltpu.make_async_copy(ids_hbm, ids_all.at[me_g], ids_sem)
    gates_copy = pltpu.make_async_copy(gates_hbm, gates, gates_sem)
    for copy in (own_copy, ids_copy, gates_copy):
        copy.start()

    def weight_copies(source, target, sem):
        depth = min(DEPTH, source.shape[0])
        groups = []
        for n in range(source.shape[0] // depth):
            rows = pl.ds(n * depth, depth)
            groups.append([
                pltpu.make_async_copy(
                    source.at[rows, pl.ds(c * LANES, LANES)], target.at[c, rows], sem.at[n, c]
                )
                for c in range(tiles)
            ])
        return groups

    shared_groups = weight_copies(
        shared_gate_up.reshape(2 * columns, units), w_shared, shared_w_sem
    )
    routed_groups = weight_copies(gate_up.reshape(2 * width, units), w_routed, routed_w_sem)
    shared_down_copy = pltpu.make_async_copy(shared_down, w_shared_down, shared_down_w_sem)
    down_copies = [
        pltpu.make_async_copy(
            down.at[0, :, pl.ds(pl.multiple_of(expert_at(-d) * columns, LANES), columns)],
            w_down.at[d],
            down_w_sem.at[d],
        )
        for d in range(n_expert)
    ]
    with scope("own"):
        own_copy.wait()
    for group in shared_groups:
        for copy in group:
            copy.start()
    shared_down_copy.start()
    with scope("bar"):
        pl.semaphore_wait(barrier, n_expert * n_group - 1)

    def x_copy(source, target, c, send_sem):
        return pltpu.make_async_remote_copy(
            src_ref=x_all.at[source, :, chunks[c]], dst_ref=x_all.at[source, :, chunks[c]],
            send_sem=send_sem, recv_sem=x_recv.at[source, c],
            device_id={"group": target}, device_id_type=MESH,
        )

    has_left, has_right = me_g > 0, me_g < n_group - 1
    sends = []
    for step, exists in ((-1, has_left), (1, has_right)):
        for c in range(parts):
            copy = x_copy(me_g, me_g + step, c, x_send.at[max(step, 0), c])
            pl.when(exists)(copy.start)
            sends.append((exists, copy))

    with scope("ids"):
        ids_copy.wait()
    ids_copies = []
    for s in range(1, n_group):
        copy = pltpu.make_async_remote_copy(
            src_ref=ids_all.at[me_g], dst_ref=ids_all.at[me_g],
            send_sem=ids_send.at[s], recv_sem=ids_recv.at[s],
            device_id={"group": group_at(s)}, device_id_type=MESH,
        )
        copy.start()
        ids_copies.append(copy)

    before = (
        lax.broadcasted_iota(jnp.int32, (n_tokens, n_tokens), 0)
        < lax.broadcasted_iota(jnp.int32, (n_tokens, n_tokens), 1)
    ).astype(BF16)
    ranks = lax.broadcasted_iota(jnp.int32, (8, n_tokens), 0).astype(F32)

    def picked_by(ids, expert):
        chosen = ids == expert
        named = jnp.sum(jnp.where(chosen, 1.0, 0.0), axis=0, keepdims=True)
        named = jnp.broadcast_to(named, (8, n_tokens))
        rank = jnp.dot(named.astype(BF16), before, preferred_element_type=F32)
        picked = jnp.where((named > 0.5) & (jnp.abs(rank - ranks) < 0.5), 1.0, 0.0)
        return picked, chosen

    feature = lax.broadcasted_iota(jnp.int32, (LANES, 4 * LANES), 0)
    place = lax.broadcasted_iota(jnp.int32, (LANES, 4 * LANES), 1)
    spread = (
        (place == 2 * feature) | (place == 2 * feature + 1 + 2 * LANES)
    ).astype(BF16)

    def expand(pieces, target):
        rows = pieces[0].shape[0]
        stacked = jnp.concatenate(pieces, axis=0).astype(BF16)
        both = jnp.dot(stacked, spread, preferred_element_type=F32).astype(BF16)
        for j in range(len(pieces)):
            at = pl.ds(j * 2 * LANES, 2 * LANES)
            target[:rows, at] = both[j * rows : (j + 1) * rows, : 2 * LANES]
            target[rows:, at] = both[j * rows : (j + 1) * rows, 2 * LANES :]

    def project(x, weights, groups, wait):
        depth = min(DEPTH, x.shape[1]) if wait else x.shape[1]
        totals = [None] * (tiles // pair)
        for n in range(x.shape[1] // depth):
            if wait:
                with scope(f"w{n}"):
                    for copy in groups[n]:
                        copy.wait()
            rows = pl.ds(n * depth, depth)
            x_part = x[:, pl.ds(n * depth, depth)]
            for p in range(tiles // pair):
                block = [weights[p * pair + i, rows] for i in range(pair)]
                block = jnp.concatenate(block, axis=1) if pair > 1 else block[0]
                product = jnp.dot(x_part, block, preferred_element_type=F32)
                totals[p] = product if totals[p] is None else totals[p] + product
        return totals

    pre_copies = {}

    def pre(k):
        source = sources[k]
        with scope(f"exp{k}"):
          expand([x_all[source, :, pl.ds(j * LANES, LANES)] for j in range(columns // LANES)], x_shared)
        with scope(f"proj{k}"):
            totals = project(x_shared, w_shared, shared_groups, k == 0)
        for p, total in enumerate(totals):
            at = pl.ds(p * pair * LANES, pair * LANES)
            pre_own[k, :, at] = total
            pre_out[k, :, at] = total.astype(BF16)
        pre_copies[k] = []
        for d in range(1, n_expert):
            copy = pltpu.make_async_remote_copy(
                src_ref=pre_out.at[k], dst_ref=pre_in.at[d - 1, k],
                send_sem=pre_send.at[d - 1, k], recv_sem=pre_recv.at[d - 1, k],
                device_id={"expert": expert_at(d)}, device_id_type=MESH,
            )
            copy.start()
            pre_copies[k].append(copy)

    term_copies = []

    def fin(k):
        with scope(f"prew{k}"):
            for copy in pre_copies[k]:
                copy.wait_recv()
        total = pre_own[k]
        for d in range(1, n_expert):
            total = total + pre_in[d - 1, k].astype(F32)
        hidden = (silu(total[:n_tokens]) * total[n_tokens:]).astype(BF16)
        for c in range(parts):
            term = jnp.dot(hidden, w_shared_down[:, chunks[c]], preferred_element_type=F32)
            if k:
                term_out[k, :, chunks[c]] = term.astype(BF16)
                copy = pltpu.make_async_remote_copy(
                    src_ref=term_out.at[k, :, chunks[c]], dst_ref=term_in.at[me_g, :, chunks[c]],
                    send_sem=term_send.at[k, c], recv_sem=term_recv.at[me_g, c],
                    device_id={"group": sources[k]}, device_id_type=MESH,
                )
                copy.start()
                term_copies.append(copy)
            else:
                term_in[me_g, :, chunks[c]] = term.astype(BF16)

    pre(0)

    for group in routed_groups:
        for copy in group:
            copy.start()
    for copy in down_copies:
        copy.start()

    relays = []

    def arrive(distance):
        for c in range(parts):
            for side in (0, 1):
                source = me_g + distance if side else me_g - distance
                target = me_g - 1 if side else me_g + 1
                exists = source < n_group if side else source >= 0
                passed = exists & (target >= 0 if side else target < n_group)
                relay = x_copy(source, target, c, relay_send.at[side, distance - 1, c])
                with scope(f"x{distance}{side}{c}"):
                    pl.when(exists)(relay.wait_recv)
                pl.when(passed)(relay.start)
                relays.append((passed, relay))

    rows_copies = []

    def select():
        for copy in ids_copies:
            copy.wait_recv()
        for s in range(n_group):
            source = group_at(-s)
            picked = jnp.concatenate(
                [picked_by(ids_all[source], expert_at(d))[0] for d in range(n_expert)], axis=0
            ).astype(BF16)
            rows = jnp.dot(picked, x_all[source], preferred_element_type=F32)
            for d in range(n_expert):
                target = rows_out.at[d, s] if d else rows_all.at[me_e, s]
                target[...] = rows[d * 8 : d * 8 + CAP].astype(BF16)
        for d in range(1, n_expert):
            copy = pltpu.make_async_remote_copy(
                src_ref=rows_out.at[d], dst_ref=rows_all.at[me_e],
                send_sem=rows_send.at[d], recv_sem=rows_recv.at[d],
                device_id={"expert": expert_at(d)}, device_id_type=MESH,
            )
            copy.start()
            rows_copies.append(copy)

    shared_down_waited = False
    for k in range(1, n_group):
        arrive(k)
        if k == n_group - 1:
            with scope("select"):
                select()
        pre(k)
        if k > 1:
            if not shared_down_waited:
                shared_down_copy.wait()
                shared_down_waited = True
            fin(k - 1)
    if not shared_down_waited:
        shared_down_copy.wait()

    with scope("rows"):
        for copy in rows_copies:
            copy.wait_recv()
    routed_rows = n_group * CAP
    with scope("rexp"):
      expand(
        [
            rows_all[h, :, :, pl.ds(j * LANES, LANES)].reshape(routed_rows, LANES).astype(F32)
            for h in range(n_expert)
            for j in range(columns // LANES)
        ],
        x_routed,
    )
    if n_group > 1:
        fin(n_group - 1)
    with scope("rproj"):
        totals = project(x_routed, w_routed, routed_groups, True)
    routed_hidden = jnp.concatenate(
        [(silu(t[:routed_rows]) * t[routed_rows:]).astype(BF16) for t in totals], axis=1
    )

    routed_copies = []
    for d in reversed(range(n_expert)):
        with scope(f"dw{d}"):
            down_copies[d].wait()
        for c in range(parts):
            term = jnp.dot(
                routed_hidden, w_down[d, :, chunks[c]], preferred_element_type=F32
            ).astype(BF16)
            for s in range(n_group):
                rows = term[s * CAP : (s + 1) * CAP]
                if d or s:
                    routed_out[d, s, :, chunks[c]] = rows
                else:
                    routed_in[0, 0, :, chunks[c]] = rows
        for s in list(range(1, n_group)) + [0]:
            if d or s:
                copy = pltpu.make_async_remote_copy(
                    src_ref=routed_out.at[d, s], dst_ref=routed_in.at[d, s],
                    send_sem=routed_send.at[d, s], recv_sem=routed_recv.at[d, s],
                    device_id={"expert": expert_at(-d), "group": group_at(-s)},
                    device_id_type=MESH,
                )
                copy.start()
                routed_copies.append(copy)
    fin(0)

    identity = (
        lax.broadcasted_iota(jnp.int32, (n_tokens, n_tokens), 0)
        == lax.broadcasted_iota(jnp.int32, (n_tokens, n_tokens), 1)
    ).astype(BF16)
    gates_copy.wait()
    weights = []
    for d in range(n_expert):
        picked, chosen = picked_by(ids_all[me_g], expert_at(d))
        value = jnp.sum(jnp.where(chosen, gates[...].astype(F32), 0.0), axis=0, keepdims=True)
        weights.append(lax.dot_general(
            identity, (picked * value).astype(BF16), (((1,), (1,)), ((), ())),
            preferred_element_type=F32,
        ))
    with scope("routed"):
        for copy in routed_copies:
            copy.wait_recv()
    for c in range(parts):
        for s in range(n_group):
            copy = pltpu.make_async_remote_copy(
                src_ref=term_out.at[0, :, chunks[c]], dst_ref=term_in.at[s, :, chunks[c]],
                send_sem=term_send.at[0, c], recv_sem=term_recv.at[s, c],
                device_id={"group": group_at(1)}, device_id_type=MESH,
            )
            with scope(f"term{c}{s}"):
                pl.when(me_g != s)(copy.wait_recv)
        at = chunks[c]
        total = term_in[0, :, at].astype(F32)
        for s in range(1, n_group):
            total = total + term_in[s, :, at].astype(F32)
        for d in range(n_expert):
            rows = routed_in[d, 0, :, at].astype(F32)
            for s in range(1, n_group):
                rows = rows + routed_in[d, s, :, at].astype(F32)
            for r in range(CAP):
                total = total + weights[d][:, r : r + 1] * rows[r : r + 1]
        out[:, at] = total.astype(BF16)

    with scope("sendw"):
      for exists, copy in sends + relays:
        pl.when(exists)(copy.wait_send)
    for copy in ids_copies + rows_copies + term_copies + routed_copies:
        copy.wait_send()
    for copies in pre_copies.values():
        for copy in copies:
            copy.wait_send()


def per_device(n_expert, n_group, tokens, ids, gates, gate_up, down, shared_gate_up, shared_down):
    n_tokens, width = tokens.shape
    columns, _, units = shared_gate_up.shape
    tiles = units // LANES
    top = ids.shape[1]
    parts = 2 if columns % (2 * LANES) == 0 else 1
    vmem, dma = pltpu.VMEM, pltpu.SemaphoreType.DMA
    in_vmem, in_hbm = pl.BlockSpec(memory_space=pltpu.VMEM), pl.BlockSpec(memory_space=pltpu.HBM)
    return pl.pallas_call(
        functools.partial(kernel, n_expert, n_group),
        out_shape=jax.ShapeDtypeStruct((n_tokens, columns), BF16),
        in_specs=[in_hbm] * 7,
        out_specs=in_vmem,
        scratch_shapes=[
            vmem((tiles, 2 * width, LANES), BF16),
            vmem((n_expert, units, columns), BF16),
            vmem((tiles, 2 * columns, LANES), BF16),
            vmem((units, columns), BF16),
            vmem((n_group, top, n_tokens), jnp.int32),
            vmem((top, n_tokens), BF16),
            vmem((n_group, n_tokens, columns), BF16),
            vmem((2 * n_tokens, 2 * columns), BF16),
            vmem((n_expert, n_group, CAP, columns), BF16),
            vmem((n_expert, n_group, CAP, columns), BF16),
            vmem((2 * n_group * CAP, 2 * width), BF16),
            vmem((n_group, 2 * n_tokens, units), F32),
            vmem((n_group, 2 * n_tokens, units), BF16),
            vmem((max(1, n_expert - 1), n_group, 2 * n_tokens, units), BF16),
            vmem((n_group, n_tokens, columns), BF16),
            vmem((n_group, n_tokens, columns), BF16),
            vmem((n_expert, n_group, CAP, columns), BF16),
            vmem((n_expert, n_group, CAP, columns), BF16),
            dma((max(1, 2 * width // DEPTH), tiles)),
            dma((n_expert,)),
            dma((max(1, 2 * columns // DEPTH), tiles)),
            dma, dma, dma, dma,
            dma((2, parts)), dma((n_group, parts)), dma((2, n_group, parts)),
            dma((n_group,)), dma((n_group,)),
            dma((n_expert,)), dma((n_expert,)),
            dma((max(1, n_expert - 1), n_group)), dma((max(1, n_expert - 1), n_group)),
            dma((n_group, parts)), dma((n_group, parts)),
            dma((n_expert, n_group)), dma((n_expert, n_group)),
        ],
        compiler_params=pltpu.CompilerParams(
            collective_id=0, has_side_effects=True, vmem_limit_bytes=42 * 2**20
        ),
    )(*(
        pltpu.with_memory_space_constraint(array, pltpu.HBM)
        for array in (tokens, ids.T, gates.T, gate_up, down, shared_gate_up, shared_down)
    ))


def solution(mesh):
    in_specs = (
        P(("dp", "group"), None),
        P(("dp", "group"), None),
        P(("dp", "group"), None),
        P("expert", None, None, "group"),
        P("expert", "group", None),
        P("expert", None, "group"),
        P("group", "expert"),
    )
    return jax.shard_map(
        functools.partial(per_device, mesh.shape["expert"], mesh.shape["group"]),
        mesh=mesh, in_specs=in_specs, out_specs=P(("dp", "group"), "expert"), check_vma=False,
    )
```

```python
import functools

import jax
import jax.numpy as jnp
from jax import lax
from jax.experimental import pallas as pl
from jax.experimental.pallas import tpu as pltpu
from jax.sharding import PartitionSpec as P

MESH = pl.DeviceIdType.MESH
BF16, F32 = jnp.bfloat16, jnp.float32
CAP = 2
LANES = 128
DEPTH = 1792
scope = jax.named_scope


def line_order(count):
    orders, stages = [], [[] for _ in range(count)]
    for me in range(count):
        others = [j for j in range(count) if j != me]
        orders.append([me] + sorted(others, key=lambda j: me - j if j < me else j - me + 1.5))
    for k in range(1, count):
        lists = []
        for me in range(count):
            blocks = []
            for j in sorted(range(count), key=lambda j: abs(j - me)):
                turn = orders[me].index(j)
                if j != me and k == (min(turn, abs(j - me)) if 0 < me < count - 1 else turn):
                    blocks.append(j)
            lists.append(blocks)
        for i in range(max(len(blocks) for blocks in lists)):
            stages[k].append([blocks[i] if i < len(blocks) else -1 for blocks in lists])
    return [[orders[me][k] for me in range(count)] for k in range(count)], stages


def choose(table, me):
    value = jnp.int32(0)
    for j, entry in enumerate(table):
        value = value + jnp.where(me == j, entry, 0)
    return value


def silu(value):
    return value / (1.0 + jnp.exp(-value))


def kernel(
    n_expert, n_group,
    tokens, ids_hbm, gates_hbm, gate_up, down, shared_gate_up, shared_down,
    out,
    w_routed, w_down, w_shared, w_shared_down,
    ids_all, gates,
    x_all, x_shared, rows_out, rows_all, x_routed,
    pre_own, pre_out, pre_in, term_out, term_in, routed_out, routed_in,
    routed_w_sem, down_w_sem, shared_w_sem, shared_down_w_sem, own_sem, ids_sem, gates_sem,
    ready, x_send, x_recv, relay_send, rows_send, rows_recv, pre_send, pre_recv,
    term_send, term_recv, routed_send, routed_recv,
):
    me_e, me_g = lax.axis_index("expert"), lax.axis_index("group")
    n_tokens, width = tokens.shape
    columns = x_all.shape[2]
    units = w_shared_down.shape[0]
    tiles = units // LANES
    pair = 2 if tiles % 2 == 0 else 1
    parts = 2 if columns % (2 * LANES) == 0 else 1
    part = columns // parts
    chunks = [pl.ds(c * part, part) for c in range(parts)]
    x_parts = x_recv.shape[1] - 1
    x_part = columns // x_parts
    x_chunks = [pl.ds(c * x_part, x_part) for c in range(x_parts)]
    order, stages = line_order(n_group)
    sources = [choose(table, me_g) for table in order]

    def expert_at(distance):
        return lax.rem(me_e + n_expert + distance, n_expert)

    def group_at(distance):
        return lax.rem(me_g + n_group + distance, n_group)

    has_left, has_right = me_g > 0, me_g < n_group - 1
    barrier = pltpu.get_barrier_semaphore()
    for d in range(1, n_expert):
        pl.semaphore_signal(barrier, inc=1, device_id={"expert": expert_at(d)}, device_id_type=MESH)

    @pl.when(has_right)
    def _():
        pl.semaphore_signal(barrier, inc=1, device_id={"group": me_g + 1}, device_id_type=MESH)

    own_columns = pl.ds(pl.multiple_of(me_e * columns, LANES), columns)
    own_copy = pltpu.make_async_copy(tokens.at[:, own_columns], x_all.at[me_g], own_sem)
    ids_copy = pltpu.make_async_copy(ids_hbm, ids_all.at[me_g], ids_sem)
    gates_copy = pltpu.make_async_copy(gates_hbm, gates, gates_sem)
    for copy in (own_copy, ids_copy, gates_copy):
        copy.start()

    def weight_copies(source, target, sem, first, at, count):
        depth = min(DEPTH, count)
        groups = []
        for n in range(count // depth):
            rows = pl.ds(pl.multiple_of(first + n * depth, LANES), depth)
            landed = pl.ds(at + n * depth, depth)
            copies = [
                pltpu.make_async_copy(
                    source.at[rows, pl.ds(c * LANES, LANES)], target.at[c, landed], sem.at[at // depth + n]
                )
                for c in range(tiles)
            ]
            whole = target.at[:, landed]
            groups.append((copies, pltpu.make_async_copy(whole, whole, sem.at[at // depth + n])))
        return groups

    half = 2 * columns
    shared_groups = weight_copies(
        shared_gate_up.reshape(half, units), w_shared, shared_w_sem, 0, 0, half
    )
    routed_groups = [
        weight_copies(
            gate_up.reshape(2 * width, units), w_routed, routed_w_sem, expert_at(h) * half, h * half, half
        )
        for h in range(n_expert)
    ]
    shared_down_copy = pltpu.make_async_copy(shared_down, w_shared_down, shared_down_w_sem)
    down_copies = [
        pltpu.make_async_copy(
            down.at[0, :, pl.ds(pl.multiple_of(expert_at(-d) * columns, LANES), columns)],
            w_down.at[d],
            down_w_sem.at[d],
        )
        for d in range(n_expert)
    ]
    with scope("own"):
        own_copy.wait()
    for copies, _ in shared_groups:
        for copy in copies:
            copy.start()
    shared_down_copy.start()
    with scope("bar"):
        pl.semaphore_wait(barrier, n_expert - 1 + jnp.where(has_left, 1, 0))

    @pl.when(has_left)
    def _():
        pl.semaphore_signal(ready, inc=1, device_id={"group": me_g - 1}, device_id_type=MESH)

    with scope("ids"):
        ids_copy.wait()

    def x_copy(source, target, c, send_sem):
        ref = x_all.at[source, :, x_chunks[c]] if c < x_parts else ids_all.at[source]
        return pltpu.make_async_remote_copy(
            src_ref=ref, dst_ref=ref, send_sem=send_sem, recv_sem=x_recv.at[source, c],
            device_id={"group": target}, device_id_type=MESH,
        )

    sends = []
    for i, (step, exists) in enumerate(((-1, has_left), (1, has_right))):
        if step > 0:
            with scope("ready1"):
                @pl.when(exists)
                def _():
                    pl.semaphore_wait(ready, 1)
        for c in range(x_parts + 1):
            pl.when(exists)(x_copy(me_g, me_g + step, c, x_send.at[i, c // x_parts]).start)
        sends.append((exists, x_send.at[i]))

    before = (
        lax.broadcasted_iota(jnp.int32, (n_tokens, n_tokens), 0)
        < lax.broadcasted_iota(jnp.int32, (n_tokens, n_tokens), 1)
    ).astype(BF16)
    ranks = lax.broadcasted_iota(jnp.int32, (8, n_tokens), 0).astype(F32)

    def picked_by(ids, expert):
        chosen = ids == expert
        named = jnp.sum(jnp.where(chosen, 1.0, 0.0), axis=0, keepdims=True)
        named = jnp.broadcast_to(named, (8, n_tokens))
        rank = jnp.dot(named.astype(BF16), before, preferred_element_type=F32)
        picked = jnp.where((named > 0.5) & (jnp.abs(rank - ranks) < 0.5), 1.0, 0.0)
        return picked, chosen

    feature = lax.broadcasted_iota(jnp.int32, (LANES, 4 * LANES), 0)
    place = lax.broadcasted_iota(jnp.int32, (LANES, 4 * LANES), 1)
    spread = (
        (place == 2 * feature) | (place == 2 * feature + 1 + 2 * LANES)
    ).astype(BF16)

    def expand(pieces, target):
        rows = pieces[0].shape[0]
        stacked = jnp.concatenate(pieces, axis=0).astype(BF16)
        both = jnp.dot(stacked, spread, preferred_element_type=F32).astype(BF16)
        for j in range(len(pieces)):
            at = pl.ds(j * 2 * LANES, 2 * LANES)
            target[:rows, at] = both[j * rows : (j + 1) * rows, : 2 * LANES]
            target[rows:, at] = both[j * rows : (j + 1) * rows, 2 * LANES :]

    def project(x, weights, groups, wait, first=0):
        depth = min(DEPTH, x.shape[1]) if wait else x.shape[1]
        totals = [None] * (tiles // pair)
        for n in range(x.shape[1] // depth):
            if wait:
                with scope(f"w{n}"):
                    groups[n][1].wait()
            rows = pl.ds(first + n * depth, depth)
            x_part = x[:, pl.ds(n * depth, depth)]
            for p in range(tiles // pair):
                block = [weights[p * pair + i, rows] for i in range(pair)]
                block = jnp.concatenate(block, axis=1) if pair > 1 else block[0]
                product = jnp.dot(x_part, block, preferred_element_type=F32)
                totals[p] = product if totals[p] is None else totals[p] + product
        return totals

    pre_copies = {}

    def pre(k):
        source = sources[k]
        with scope(f"exp{k}"):
          expand([x_all[source, :, pl.ds(j * LANES, LANES)] for j in range(columns // LANES)], x_shared)
        with scope(f"proj{k}"):
            totals = project(x_shared, w_shared, shared_groups, k == 0)
        for p, total in enumerate(totals):
            at = pl.ds(p * pair * LANES, pair * LANES)
            pre_own[k, :, at] = total
            pre_out[k, :, at] = total.astype(BF16)
        pre_copies[k] = []
        for d in range(1, n_expert):
            copy = pltpu.make_async_remote_copy(
                src_ref=pre_out.at[k], dst_ref=pre_in.at[d - 1, k],
                send_sem=pre_send.at[d - 1], recv_sem=pre_recv.at[d - 1, k],
                device_id={"expert": expert_at(d)}, device_id_type=MESH,
            )
            copy.start()
            pre_copies[k].append(copy)

    def fin(k):
        with scope(f"prew{k}"):
            for copy in pre_copies[k]:
                copy.wait_recv()
        total = pre_own[k]
        for d in range(1, n_expert):
            total = total + pre_in[d - 1, k].astype(F32)
        hidden = (silu(total[:n_tokens]) * total[n_tokens:]).astype(BF16)
        for c in range(parts):
            term = jnp.dot(hidden, w_shared_down[:, chunks[c]], preferred_element_type=F32)
            if k:
                term_out[k, :, chunks[c]] = term.astype(BF16)
                copy = pltpu.make_async_remote_copy(
                    src_ref=term_out.at[k, :, chunks[c]], dst_ref=term_in.at[me_g, :, chunks[c]],
                    send_sem=term_send, recv_sem=term_recv.at[me_g],
                    device_id={"group": sources[k]}, device_id_type=MESH,
                )
                copy.start()
            else:
                term_in[me_g, :, chunks[c]] = term.astype(BF16)

    pre(0)

    for groups in routed_groups:
        for copies, _ in groups:
            for copy in copies:
                copy.start()
    for copy in down_copies:
        copy.start()

    def arrive(k):
        for c in range(x_parts + 1):
            for i, table in enumerate(stages[k]):
                block = choose(table, me_g)
                passed = (block >= 0) & has_left & has_right
                target = jnp.where(block > me_g, me_g - 1, me_g + 1)
                sem = relay_send.at[sum(len(tables) for tables in stages[:k]) + i]
                relay = x_copy(block, target, c, sem.at[c // x_parts])
                with scope(f"x{k}{i}{c}"):
                    pl.when(block >= 0)(relay.wait_recv)
                pl.when(passed)(relay.start)
                if c == 0:
                    sends.append((passed, sem))


    def select(k):
        source = sources[k]
        picked = jnp.concatenate(
            [picked_by(ids_all[source], expert_at(d))[0] for d in range(n_expert)], axis=0
        ).astype(BF16)
        rows = jnp.dot(picked, x_all[source], preferred_element_type=F32)
        for d in range(n_expert):
            target = rows_out.at[d, k] if d else rows_all.at[0, k]
            target[...] = rows[d * 8 : d * 8 + CAP].astype(BF16)
        for d in range(1, n_expert):
            copy = pltpu.make_async_remote_copy(
                src_ref=rows_out.at[d, k], dst_ref=rows_all.at[n_expert - d, k],
                send_sem=rows_send.at[d], recv_sem=rows_recv.at[d],
                device_id={"expert": expert_at(d)}, device_id_type=MESH,
            )
            copy.start()

    routed_rows = n_group * CAP
    routed_totals = [None] * (tiles // pair)

    def project_rows(h):
        x = x_routed.at[min(h, 1)]
        with scope(f"rexp{h}"):
            pieces = [
                rows_all[h, :, :, pl.ds(j * LANES, LANES)].reshape(routed_rows, LANES).astype(F32)
                for j in range(columns // LANES)
            ]
            expand(pieces, x)
        with scope(f"rproj{h}"):
            totals = project(x, w_routed, routed_groups[h], True, h * half)
        for p, total in enumerate(totals):
            routed_totals[p] = total if routed_totals[p] is None else routed_totals[p] + total

    for k in range(1, n_group):
        arrive(k)
        pre(k)
        with scope("select"):
            if k == 1:
                select(0)
            select(k)
        if k == 2:
            shared_down_copy.wait()
        if k > 1:
            fin(k - 1)
        if k == n_group - 1:
            project_rows(0)
    if n_group < 3:
        shared_down_copy.wait()
    if n_group < 2:
        select(0)
        project_rows(0)
    else:
        fin(n_group - 1)
    with scope("rows"):
        for d in range(1, n_expert):
            rows = rows_all.at[n_expert - d]
            pltpu.make_async_remote_copy(
                src_ref=rows, dst_ref=rows, send_sem=rows_send.at[d], recv_sem=rows_recv.at[d],
                device_id={"expert": expert_at(d)}, device_id_type=MESH,
            ).wait_recv()
    for h in range(1, n_expert):
        project_rows(h)
    routed_hidden = jnp.concatenate(
        [(silu(t[:routed_rows]) * t[routed_rows:]).astype(BF16) for t in routed_totals], axis=1
    )

    for d in reversed(range(n_expert)):
        with scope(f"dw{d}"):
            down_copies[d].wait()
        for c in range(parts):
            term = jnp.dot(
                routed_hidden, w_down[d, :, chunks[c]], preferred_element_type=F32
            ).astype(BF16)
            for k in range(n_group):
                rows = term[k * CAP : (k + 1) * CAP]
                if d or k:
                    routed_out[d, k, :, chunks[c]] = rows
                else:
                    routed_in[0, me_g, :, chunks[c]] = rows
        for k in list(range(1, n_group)) + [0]:
            if d or k:
                copy = pltpu.make_async_remote_copy(
                    src_ref=routed_out.at[d, k], dst_ref=routed_in.at[d, me_g],
                    send_sem=routed_send.at[d], recv_sem=routed_recv.at[d],
                    device_id={"expert": expert_at(-d), "group": sources[k]},
                    device_id_type=MESH,
                )
                copy.start()
    fin(0)

    identity = (
        lax.broadcasted_iota(jnp.int32, (n_tokens, n_tokens), 0)
        == lax.broadcasted_iota(jnp.int32, (n_tokens, n_tokens), 1)
    ).astype(BF16)
    gates_copy.wait()
    weights = []
    for d in range(n_expert):
        picked, chosen = picked_by(ids_all[me_g], expert_at(d))
        value = jnp.sum(jnp.where(chosen, gates[...].astype(F32), 0.0), axis=0, keepdims=True)
        weights.append(lax.dot_general(
            identity, (picked * value).astype(BF16), (((1,), (1,)), ((), ())),
            preferred_element_type=F32,
        ))

    def came(ref, sem):
        return pltpu.make_async_remote_copy(
            src_ref=ref, dst_ref=ref, send_sem=sem, recv_sem=sem,
            device_id={"group": group_at(1)}, device_id_type=MESH,
        )

    for s in range(n_group):
        with scope(f"term0{s}"):
            pl.when(me_g != s)(came(term_in.at[s], term_recv.at[s]).wait_recv)
    with scope("routed"):
        for d in range(1, n_expert):
            came(routed_in.at[d], routed_recv.at[d]).wait_recv()
        if n_group > 1:
            came(routed_in.at[0, pl.ds(1, n_group - 1)], routed_recv.at[0]).wait_recv()
    for c in range(parts):
        at = chunks[c]
        total = term_in[0, :, at].astype(F32)
        for s in range(1, n_group):
            total = total + term_in[s, :, at].astype(F32)
        for d in range(n_expert):
            rows = routed_in[d, 0, :, at].astype(F32)
            for s in range(1, n_group):
                rows = rows + routed_in[d, s, :, at].astype(F32)
            for r in range(CAP):
                total = total + weights[d][:, r : r + 1] * rows[r : r + 1]
        out[:, at] = total.astype(BF16)

    with scope("sendw"):
        for exists, sem in sends:
            pl.when(exists)(came(x_all.at[0], sem.at[0]).wait_send)
            pl.when(exists)(came(ids_all.at[0], sem.at[1]).wait_send)
        for d in range(1, n_expert):
            came(rows_out.at[d], rows_send.at[d]).wait_send()
            came(pre_out, pre_send.at[d - 1]).wait_send()
            came(routed_out.at[d], routed_send.at[d]).wait_send()
        if n_group > 1:
            came(term_out.at[pl.ds(1, n_group - 1)], term_send).wait_send()
            came(routed_out.at[0, pl.ds(1, n_group - 1)], routed_send.at[0]).wait_send()


def per_device(n_expert, n_group, tokens, ids, gates, gate_up, down, shared_gate_up, shared_down):
    n_tokens, width = tokens.shape
    columns, _, units = shared_gate_up.shape
    tiles = units // LANES
    top = ids.shape[1]
    parts = 2 if columns % (2 * LANES) == 0 else 1
    n_stages = max(1, sum(len(tables) for tables in line_order(n_group)[1]))
    vmem, dma = pltpu.VMEM, pltpu.SemaphoreType.DMA
    in_vmem, in_hbm = pl.BlockSpec(memory_space=pltpu.VMEM), pl.BlockSpec(memory_space=pltpu.HBM)
    return pl.pallas_call(
        functools.partial(kernel, n_expert, n_group),
        out_shape=jax.ShapeDtypeStruct((n_tokens, columns), BF16),
        in_specs=[in_hbm] * 7,
        out_specs=in_vmem,
        scratch_shapes=[
            vmem((tiles, 2 * width, LANES), BF16),
            vmem((n_expert, units, columns), BF16),
            vmem((tiles, 2 * columns, LANES), BF16),
            vmem((units, columns), BF16),
            vmem((n_group, top, n_tokens), jnp.int32),
            vmem((top, n_tokens), BF16),
            vmem((n_group, n_tokens, columns), BF16),
            vmem((2 * n_tokens, 2 * columns), BF16),
            vmem((n_expert, n_group, CAP, columns), BF16),
            vmem((n_expert, n_group, CAP, columns), BF16),
            vmem((2, 2 * n_group * CAP, 2 * columns), BF16),
            vmem((n_group, 2 * n_tokens, units), F32),
            vmem((n_group, 2 * n_tokens, units), BF16),
            vmem((max(1, n_expert - 1), n_group, 2 * n_tokens, units), BF16),
            vmem((n_group, n_tokens, columns), BF16),
            vmem((n_group, n_tokens, columns), BF16),
            vmem((n_expert, n_group, CAP, columns), BF16),
            vmem((n_expert, n_group, CAP, columns), BF16),
            dma((2 * width // min(DEPTH, 2 * columns),)),
            dma((n_expert,)),
            dma((2 * columns // min(DEPTH, 2 * columns),)),
            dma, dma, dma, dma,
            pltpu.SemaphoreType.REGULAR,
            dma((2, 2)), dma((n_group, parts + 1)), dma((n_stages, 2)),
            dma((n_expert,)), dma((n_expert,)),
            dma((max(1, n_expert - 1),)), dma((max(1, n_expert - 1), n_group)),
            dma, dma((n_group,)),
            dma((n_expert,)), dma((n_expert,)),
        ],
        compiler_params=pltpu.CompilerParams(
            collective_id=0, has_side_effects=True, vmem_limit_bytes=42 * 2**20
        ),
    )(*(
        pltpu.with_memory_space_constraint(array, pltpu.HBM)
        for array in (tokens, ids.T, gates.T, gate_up, down, shared_gate_up, shared_down)
    ))


def solution(mesh):
    in_specs = (
        P(("dp", "group"), None),
        P(("dp", "group"), None),
        P(("dp", "group"), None),
        P("expert", None, None, "group"),
        P("expert", "group", None),
        P("expert", None, "group"),
        P("group", "expert"),
    )
    return jax.shard_map(
        functools.partial(per_device, mesh.shape["expert"], mesh.shape["group"]),
        mesh=mesh, in_specs=in_specs, out_specs=P(("dp", "group"), "expert"), check_vma=False,
    )
```

```python
import functools

import jax
import jax.numpy as jnp
from jax import lax
from jax.experimental import pallas as pl
from jax.experimental.pallas import tpu as pltpu
from jax.sharding import PartitionSpec as P

MESH = pl.DeviceIdType.MESH
BF16, F32 = jnp.bfloat16, jnp.float32
CAP = 2
LANES = 128
DEPTH = 1792
scope = jax.named_scope


def line_order(count):
    orders, stages = [], [[] for _ in range(count)]
    for me in range(count):
        others = [j for j in range(count) if j != me]
        orders.append([me] + sorted(others, key=lambda j: me - j if j < me else j - me + 1.5))
    for k in range(1, count):
        lists = []
        for me in range(count):
            blocks = []
            for j in sorted(range(count), key=lambda j: abs(j - me)):
                turn = orders[me].index(j)
                if j != me and k == (min(turn, abs(j - me)) if 0 < me < count - 1 else turn):
                    blocks.append(j)
            lists.append(blocks)
        for i in range(max(len(blocks) for blocks in lists)):
            stages[k].append([blocks[i] if i < len(blocks) else -1 for blocks in lists])
    return [[orders[me][k] for me in range(count)] for k in range(count)], stages


def choose(table, me):
    value = jnp.int32(0)
    for j, entry in enumerate(table):
        value = value + jnp.where(me == j, entry, 0)
    return value


def silu(value):
    return value / (1.0 + jnp.exp(-value))


def kernel(
    n_expert, n_group,
    tokens, ids_hbm, gates_hbm, gate_up, down, shared_gate_up, shared_down,
    out,
    w_routed, w_down, w_shared, w_shared_down,
    ids_all, gates,
    x_all, x_shared, rows_out, rows_all, x_routed,
    pre_own, pre_out, pre_in, term_out, term_in, routed_out, routed_in,
    routed_w_sem, down_w_sem, shared_w_sem, shared_down_w_sem, own_sem, ids_sem, gates_sem,
    ready, x_send, x_recv, relay_send, rows_send, rows_recv, pre_send, pre_recv,
    term_send, term_recv, routed_send, routed_recv,
):
    me_e, me_g = lax.axis_index("expert"), lax.axis_index("group")
    n_tokens, width = tokens.shape
    columns = x_all.shape[2]
    units = w_shared_down.shape[0]
    tiles = units // LANES
    pair = 2 if tiles % 2 == 0 else 1
    parts = 2 if columns % (2 * LANES) == 0 else 1
    part = columns // parts
    chunks = [pl.ds(c * part, part) for c in range(parts)]
    x_parts = x_recv.shape[1] - 1
    x_part = columns // x_parts
    x_chunks = [pl.ds(c * x_part, x_part) for c in range(x_parts)]
    order, stages = line_order(n_group)
    sources = [choose(table, me_g) for table in order]

    def expert_at(distance):
        return lax.rem(me_e + n_expert + distance, n_expert)

    def group_at(distance):
        return lax.rem(me_g + n_group + distance, n_group)

    has_left, has_right = me_g > 0, me_g < n_group - 1
    barrier = pltpu.get_barrier_semaphore()
    for d in range(1, n_expert):
        pl.semaphore_signal(barrier, inc=1, device_id={"expert": expert_at(d)}, device_id_type=MESH)

    @pl.when(has_right)
    def _():
        pl.semaphore_signal(barrier, inc=1, device_id={"group": me_g + 1}, device_id_type=MESH)

    own_columns = pl.ds(pl.multiple_of(me_e * columns, LANES), columns)
    own_copy = pltpu.make_async_copy(tokens.at[:, own_columns], x_all.at[me_g], own_sem)
    ids_copy = pltpu.make_async_copy(ids_hbm, ids_all.at[me_g], ids_sem)
    gates_copy = pltpu.make_async_copy(gates_hbm, gates, gates_sem)
    for copy in (own_copy, ids_copy, gates_copy):
        copy.start()

    with scope("bar"):
        @pl.when(has_left)
        def _():
            pl.semaphore_wait(barrier, n_expert)
            pl.semaphore_signal(ready, inc=1, device_id={"group": me_g - 1}, device_id_type=MESH)

    def weight_copies(source, target, sem, first, at, count):
        depth = min(DEPTH, count)
        groups = []
        for n in range(count // depth):
            rows = pl.ds(pl.multiple_of(first + n * depth, LANES), depth)
            landed = pl.ds(at + n * depth, depth)
            copies = [
                pltpu.make_async_copy(
                    source.at[rows, pl.ds(c * LANES, LANES)], target.at[c, landed], sem.at[at // depth + n]
                )
                for c in range(tiles)
            ]
            whole = target.at[:, landed]
            groups.append((copies, pltpu.make_async_copy(whole, whole, sem.at[at // depth + n])))
        return groups

    half = 2 * columns
    shared_groups = weight_copies(
        shared_gate_up.reshape(half, units), w_shared, shared_w_sem, 0, 0, half
    )
    routed_groups = [
        weight_copies(
            gate_up.reshape(2 * width, units), w_routed, routed_w_sem, expert_at(h) * half, h * half, half
        )
        for h in range(n_expert)
    ]
    shared_down_copy = pltpu.make_async_copy(shared_down, w_shared_down, shared_down_w_sem)
    down_copies = [
        pltpu.make_async_copy(
            down.at[0, :, pl.ds(pl.multiple_of(expert_at(-d) * columns, LANES), columns)],
            w_down.at[d],
            down_w_sem.at[d],
        )
        for d in range(n_expert)
    ]
    with scope("own"):
        own_copy.wait()
    for copies, _ in shared_groups:
        for copy in copies:
            copy.start()
    shared_down_copy.start()
    with scope("bar0"):
        @pl.when(me_g == 0)
        def _():
            pl.semaphore_wait(barrier, n_expert - 1)

    with scope("ids"):
        ids_copy.wait()

    def x_copy(source, target, c, send_sem):
        ref = x_all.at[source, :, x_chunks[c]] if c < x_parts else ids_all.at[source]
        return pltpu.make_async_remote_copy(
            src_ref=ref, dst_ref=ref, send_sem=send_sem, recv_sem=x_recv.at[source, c],
            device_id={"group": target}, device_id_type=MESH,
        )

    sends = []
    for i, (step, exists) in enumerate(((-1, has_left), (1, has_right))):
        if step > 0:
            with scope("ready1"):
                @pl.when(exists)
                def _():
                    pl.semaphore_wait(ready, 1)
        for c in range(x_parts + 1):
            pl.when(exists)(x_copy(me_g, me_g + step, c, x_send.at[i, c // x_parts]).start)
        sends.append((exists, x_send.at[i]))

    before = (
        lax.broadcasted_iota(jnp.int32, (n_tokens, n_tokens), 0)
        < lax.broadcasted_iota(jnp.int32, (n_tokens, n_tokens), 1)
    ).astype(BF16)
    ranks = lax.broadcasted_iota(jnp.int32, (8, n_tokens), 0).astype(F32)

    def picked_by(ids, expert):
        chosen = ids == expert
        named = jnp.sum(jnp.where(chosen, 1.0, 0.0), axis=0, keepdims=True)
        named = jnp.broadcast_to(named, (8, n_tokens))
        rank = jnp.dot(named.astype(BF16), before, preferred_element_type=F32)
        picked = jnp.where((named > 0.5) & (jnp.abs(rank - ranks) < 0.5), 1.0, 0.0)
        return picked, chosen

    feature = lax.broadcasted_iota(jnp.int32, (LANES, 4 * LANES), 0)
    place = lax.broadcasted_iota(jnp.int32, (LANES, 4 * LANES), 1)
    spread = (
        (place == 2 * feature) | (place == 2 * feature + 1 + 2 * LANES)
    ).astype(BF16)

    def expand(pieces, target):
        rows = pieces[0].shape[0]
        stacked = jnp.concatenate(pieces, axis=0).astype(BF16)
        both = jnp.dot(stacked, spread, preferred_element_type=F32).astype(BF16)
        for j in range(len(pieces)):
            at = pl.ds(j * 2 * LANES, 2 * LANES)
            target[:rows, at] = both[j * rows : (j + 1) * rows, : 2 * LANES]
            target[rows:, at] = both[j * rows : (j + 1) * rows, 2 * LANES :]

    def project(x, weights, groups, wait, first=0):
        depth = min(DEPTH, x.shape[1]) if wait else x.shape[1]
        totals = [None] * (tiles // pair)
        for n in range(x.shape[1] // depth):
            if wait:
                with scope(f"w{n}"):
                    groups[n][1].wait()
            rows = pl.ds(first + n * depth, depth)
            x_part = x[:, pl.ds(n * depth, depth)]
            for p in range(tiles // pair):
                block = [weights[p * pair + i, rows] for i in range(pair)]
                block = jnp.concatenate(block, axis=1) if pair > 1 else block[0]
                product = jnp.dot(x_part, block, preferred_element_type=F32)
                totals[p] = product if totals[p] is None else totals[p] + product
        return totals

    pre_copies = {}

    def pre(k):
        source = sources[k]
        with scope(f"exp{k}"):
          expand([x_all[source, :, pl.ds(j * LANES, LANES)] for j in range(columns // LANES)], x_shared)
        with scope(f"proj{k}"):
            totals = project(x_shared, w_shared, shared_groups, k == 0)
        for p, total in enumerate(totals):
            at = pl.ds(p * pair * LANES, pair * LANES)
            pre_own[k, :, at] = total
            pre_out[k, :, at] = total.astype(BF16)
        pre_copies[k] = []
        for d in range(1, n_expert):
            copy = pltpu.make_async_remote_copy(
                src_ref=pre_out.at[k], dst_ref=pre_in.at[d - 1, k],
                send_sem=pre_send.at[d - 1], recv_sem=pre_recv.at[d - 1, k],
                device_id={"expert": expert_at(d)}, device_id_type=MESH,
            )
            copy.start()
            pre_copies[k].append(copy)

    last = n_group - 1
    swapped = sources[last] < sources[last - 1]
    held = []

    def fin(k):
        with scope(f"prew{k}"):
            for copy in pre_copies[k]:
                copy.wait_recv()
        total = pre_own[k]
        for d in range(1, n_expert):
            total = total + pre_in[d - 1, k].astype(F32)
        hidden = (silu(total[:n_tokens]) * total[n_tokens:]).astype(BF16)
        for c in range(parts):
            term = jnp.dot(hidden, w_shared_down[:, chunks[c]], preferred_element_type=F32)
            if k:
                term_out[k, :, chunks[c]] = term.astype(BF16)
                copy = pltpu.make_async_remote_copy(
                    src_ref=term_out.at[k, :, chunks[c]], dst_ref=term_in.at[me_g, :, chunks[c]],
                    send_sem=term_send, recv_sem=term_recv.at[me_g],
                    device_id={"group": sources[k]}, device_id_type=MESH,
                )
                if 1 < k + 1 == last:
                    pl.when(~swapped)(copy.start)
                    held.append(copy)
                else:
                    copy.start()
            else:
                term_in[me_g, :, chunks[c]] = term.astype(BF16)

    pre(0)

    for groups in routed_groups:
        for copies, _ in groups:
            for copy in copies:
                copy.start()
    for copy in down_copies:
        copy.start()

    def arrive(k):
        for c in range(x_parts + 1):
            for i, table in enumerate(stages[k]):
                block = choose(table, me_g)
                passed = (block >= 0) & has_left & has_right
                target = jnp.where(block > me_g, me_g - 1, me_g + 1)
                sem = relay_send.at[sum(len(tables) for tables in stages[:k]) + i]
                relay = x_copy(block, target, c, sem.at[c // x_parts])
                with scope(f"x{k}{i}{c}"):
                    pl.when(block >= 0)(relay.wait_recv)
                pl.when(passed)(relay.start)
                if c == 0:
                    sends.append((passed, sem))


    def select(k):
        source = sources[k]
        picked = jnp.concatenate(
            [picked_by(ids_all[source], expert_at(d))[0] for d in range(n_expert)], axis=0
        ).astype(BF16)
        rows = jnp.dot(picked, x_all[source], preferred_element_type=F32)
        for d in range(n_expert):
            target = rows_out.at[d, k] if d else rows_all.at[0, k]
            target[...] = rows[d * 8 : d * 8 + CAP].astype(BF16)
        for d in range(1, n_expert):
            copy = pltpu.make_async_remote_copy(
                src_ref=rows_out.at[d, k], dst_ref=rows_all.at[n_expert - d, k],
                send_sem=rows_send.at[d], recv_sem=rows_recv.at[d],
                device_id={"expert": expert_at(d)}, device_id_type=MESH,
            )
            copy.start()

    routed_rows = n_group * CAP
    routed_totals = [None] * (tiles // pair)

    def project_rows(h):
        x = x_routed.at[min(h, 1)]
        with scope(f"rexp{h}"):
            pieces = [
                rows_all[h, :, :, pl.ds(j * LANES, LANES)].reshape(routed_rows, LANES).astype(F32)
                for j in range(columns // LANES)
            ]
            expand(pieces, x)
        with scope(f"rproj{h}"):
            totals = project(x, w_routed, routed_groups[h], True, h * half)
        for p, total in enumerate(totals):
            routed_totals[p] = total if routed_totals[p] is None else routed_totals[p] + total

    for k in range(1, n_group):
        arrive(k)
        pre(k)
        with scope("select"):
            if k == 1:
                select(0)
            select(k)
        if k == 2:
            shared_down_copy.wait()
        if k > 1:
            fin(k - 1)
        if k == n_group - 1:
            project_rows(0)
    if n_group < 3:
        shared_down_copy.wait()
    if n_group < 2:
        select(0)
        project_rows(0)
    else:
        fin(last)
        for copy in held:
            pl.when(swapped)(copy.start)
    with scope("rows"):
        for d in range(1, n_expert):
            rows = rows_all.at[n_expert - d]
            pltpu.make_async_remote_copy(
                src_ref=rows, dst_ref=rows, send_sem=rows_send.at[d], recv_sem=rows_recv.at[d],
                device_id={"expert": expert_at(d)}, device_id_type=MESH,
            ).wait_recv()
    for h in range(1, n_expert):
        project_rows(h)
    routed_hidden = jnp.concatenate(
        [(silu(t[:routed_rows]) * t[routed_rows:]).astype(BF16) for t in routed_totals], axis=1
    )

    for d in reversed(range(n_expert)):
        with scope(f"dw{d}"):
            down_copies[d].wait()
        for c in range(parts):
            term = jnp.dot(
                routed_hidden, w_down[d, :, chunks[c]], preferred_element_type=F32
            ).astype(BF16)
            for k in range(n_group):
                rows = term[k * CAP : (k + 1) * CAP]
                if d or k:
                    routed_out[d, k, :, chunks[c]] = rows
                else:
                    routed_in[0, me_g, :, chunks[c]] = rows
        for s in range(n_group):
            slot = choose([[row[me] for row in order].index(s) for me in range(n_group)], me_g)
            copy = pltpu.make_async_remote_copy(
                src_ref=routed_out.at[d, slot], dst_ref=routed_in.at[d, me_g],
                send_sem=routed_send.at[d], recv_sem=routed_recv.at[d],
                device_id={"expert": expert_at(-d), "group": s},
                device_id_type=MESH,
            )
            if d:
                copy.start()
            else:
                pl.when(me_g != s)(copy.start)
    fin(0)

    identity = (
        lax.broadcasted_iota(jnp.int32, (n_tokens, n_tokens), 0)
        == lax.broadcasted_iota(jnp.int32, (n_tokens, n_tokens), 1)
    ).astype(BF16)
    gates_copy.wait()
    weights = []
    for d in range(n_expert):
        picked, chosen = picked_by(ids_all[me_g], expert_at(d))
        value = jnp.sum(jnp.where(chosen, gates[...].astype(F32), 0.0), axis=0, keepdims=True)
        weights.append(lax.dot_general(
            identity, (picked * value).astype(BF16), (((1,), (1,)), ((), ())),
            preferred_element_type=F32,
        ))

    def came(ref, sem):
        return pltpu.make_async_remote_copy(
            src_ref=ref, dst_ref=ref, send_sem=sem, recv_sem=sem,
            device_id={"group": group_at(1)}, device_id_type=MESH,
        )

    for s in range(n_group):
        with scope(f"term0{s}"):
            pl.when(me_g != s)(came(term_in.at[s], term_recv.at[s]).wait_recv)
    with scope("routed"):
        for d in range(1, n_expert):
            came(routed_in.at[d], routed_recv.at[d]).wait_recv()
        if n_group > 1:
            came(routed_in.at[0, pl.ds(1, n_group - 1)], routed_recv.at[0]).wait_recv()
    for c in range(parts):
        at = chunks[c]
        total = term_in[0, :, at].astype(F32)
        for s in range(1, n_group):
            total = total + term_in[s, :, at].astype(F32)
        for d in range(n_expert):
            rows = routed_in[d, 0, :, at].astype(F32)
            for s in range(1, n_group):
                rows = rows + routed_in[d, s, :, at].astype(F32)
            for r in range(CAP):
                total = total + weights[d][:, r : r + 1] * rows[r : r + 1]
        out[:, at] = total.astype(BF16)

    with scope("sendw"):
        for exists, sem in sends:
            pl.when(exists)(came(x_all.at[0], sem.at[0]).wait_send)
            pl.when(exists)(came(ids_all.at[0], sem.at[1]).wait_send)
        for d in range(1, n_expert):
            came(rows_out.at[d], rows_send.at[d]).wait_send()
            came(pre_out, pre_send.at[d - 1]).wait_send()
            came(routed_out.at[d], routed_send.at[d]).wait_send()
        if n_group > 1:
            came(term_out.at[pl.ds(1, n_group - 1)], term_send).wait_send()
            came(routed_out.at[0, pl.ds(1, n_group - 1)], routed_send.at[0]).wait_send()


def per_device(n_expert, n_group, tokens, ids, gates, gate_up, down, shared_gate_up, shared_down):
    n_tokens, width = tokens.shape
    columns, _, units = shared_gate_up.shape
    tiles = units // LANES
    top = ids.shape[1]
    parts = 2 if columns % (2 * LANES) == 0 else 1
    n_stages = max(1, sum(len(tables) for tables in line_order(n_group)[1]))
    vmem, dma = pltpu.VMEM, pltpu.SemaphoreType.DMA
    in_vmem, in_hbm = pl.BlockSpec(memory_space=pltpu.VMEM), pl.BlockSpec(memory_space=pltpu.HBM)
    return pl.pallas_call(
        functools.partial(kernel, n_expert, n_group),
        out_shape=jax.ShapeDtypeStruct((n_tokens, columns), BF16),
        in_specs=[in_hbm] * 7,
        out_specs=in_vmem,
        scratch_shapes=[
            vmem((tiles, 2 * width, LANES), BF16),
            vmem((n_expert, units, columns), BF16),
            vmem((tiles, 2 * columns, LANES), BF16),
            vmem((units, columns), BF16),
            vmem((n_group, top, n_tokens), jnp.int32),
            vmem((top, n_tokens), BF16),
            vmem((n_group, n_tokens, columns), BF16),
            vmem((2 * n_tokens, 2 * columns), BF16),
            vmem((n_expert, n_group, CAP, columns), BF16),
            vmem((n_expert, n_group, CAP, columns), BF16),
            vmem((2, 2 * n_group * CAP, 2 * columns), BF16),
            vmem((n_group, 2 * n_tokens, units), F32),
            vmem((n_group, 2 * n_tokens, units), BF16),
            vmem((max(1, n_expert - 1), n_group, 2 * n_tokens, units), BF16),
            vmem((n_group, n_tokens, columns), BF16),
            vmem((n_group, n_tokens, columns), BF16),
            vmem((n_expert, n_group, CAP, columns), BF16),
            vmem((n_expert, n_group, CAP, columns), BF16),
            dma((2 * width // min(DEPTH, 2 * columns),)),
            dma((n_expert,)),
            dma((2 * columns // min(DEPTH, 2 * columns),)),
            dma, dma, dma, dma,
            pltpu.SemaphoreType.REGULAR,
            dma((2, 2)), dma((n_group, parts + 1)), dma((n_stages, 2)),
            dma((n_expert,)), dma((n_expert,)),
            dma((max(1, n_expert - 1),)), dma((max(1, n_expert - 1), n_group)),
            dma, dma((n_group,)),
            dma((n_expert,)), dma((n_expert,)),
        ],
        compiler_params=pltpu.CompilerParams(
            collective_id=0, has_side_effects=True, vmem_limit_bytes=42 * 2**20
        ),
    )(*(
        pltpu.with_memory_space_constraint(array, pltpu.HBM)
        for array in (tokens, ids.T, gates.T, gate_up, down, shared_gate_up, shared_down)
    ))


def solution(mesh):
    in_specs = (
        P(("dp", "group"), None),
        P(("dp", "group"), None),
        P(("dp", "group"), None),
        P("expert", None, None, "group"),
        P("expert", "group", None),
        P("expert", None, "group"),
        P("group", "expert"),
    )
    return jax.shard_map(
        functools.partial(per_device, mesh.shape["expert"], mesh.shape["group"]),
        mesh=mesh, in_specs=in_specs, out_specs=P(("dp", "group"), "expert"), check_vma=False,
    )
```
